32 devices in a mesh: data: 2 (over x), pp: 4 (over z), ep: 4 (over y, core).
Axes of the slice: x: 2, y: 2, z: 4, core: 2. Of those that a mesh axis runs over, the one named last changes fastest.
Arguments:
- O: bfloat16 [8, 6, 64, 96, 1792], P(('data', 'pp'), None, 'ep'), parts along dimension 0
- idx: int32 [8, 6, 4, 128, 8], P(('data', 'pp'), None, 'ep'), parts along dimension 0
- slot: int32 [8, 6, 4, 128, 8], P(('data', 'pp'), None, 'ep'), parts along dimension 0
- g: float32 [8, 6, 4, 128, 8], P(('data', 'pp'), None, 'ep'), parts along dimension 0
- H: bfloat16 [8, 6, 4, 128, 1792], P(('data', 'pp'), None, 'ep'), parts along dimension 0
- w: float32 [4, 1792], P('pp')
- Wq: bfloat16 [4, 1792, 32, 128], P('pp')
- Wk: bfloat16 [4, 1792, 32, 128], P('pp')
- Wv: bfloat16 [4, 1792, 32, 128], P('pp')
- Wo: bfloat16 [4, 32, 128, 1792], P('pp')
Outputs:
- output: bfloat16 [8, 6, 4, 128, 1792], P(('data', 'pp'), None, 'ep'), parts along dimension 0
There are 2 independent parts. The reference program is written for one: setup_inputs(seed, part) draws one part's arguments, and reference() takes and returns one part's arrays. A program takes and returns all parts, laid end to end along the dimension named above; an argument that names none is the same for every part.
All inputs are finite; a program needn't handle non-finite values.
Results may differ from the reference program's by a relative error of at most 0.0128283.
Values are sent between devices in bfloat16 or wider.
A program may use at most 1 GiB of HBM per device.

```python
import math
import jax
import jax.numpy as jnp
from jax import lax

PP = 4
EP = 4
M = 6
SEQ_DEV = 1
L = 128
D = 1792
HEADS = 32
HEAD_DIM = 128
EXPERTS = 64
TOP = 8
CG = 24

EPS = 1e-6
SEQS = EP * SEQ_DEV
TD = SEQ_DEV * L
T = EP * TD
C = EP * CG
QKV = HEADS * HEAD_DIM


def ranks(e, pr):
    n = e.shape[0]
    order = jnp.argsort(e * n + pr)
    se = e[order]
    start = jnp.searchsorted(se, se, side='left').astype(jnp.int32)
    r = jnp.arange(n, dtype=jnp.int32) - start
    return jnp.zeros((n,), jnp.int32).at[order].set(r)


def setup_inputs(seed: int = 0, part: int = 0) -> dict:
    ks = jax.random.split(jax.random.fold_in(jax.random.key(seed), part), 8)
    kd = jax.random.split(jax.random.fold_in(jax.random.fold_in(jax.random.key(seed), part), 7), 3)
    kw = jax.random.split(jax.random.key(seed + 1), 5)
    normal_sum = jnp.sum(jax.random.randint(kd[0], (PP, 4, EXPERTS), 0, 256), axis=1)
    octave_step = ((4 * 255 - normal_sum) // 16).astype(jnp.uint32)
    mant_table = jnp.array([256, 279, 304, 332, 362, 395, 431, 470], dtype=jnp.uint32)
    inv_weight = jnp.repeat(mant_table[octave_step & 7] << (octave_step >> 3), M, axis=0)

    def route(i):
        raw_bits = jax.random.bits(jax.random.fold_in(kd[1], i), (T, EXPERTS), jnp.uint32) >> 16
        wait_time = raw_bits * inv_weight[i]
        return jnp.argsort(wait_time, axis=-1)[:, :TOP].astype(jnp.int32)

    idx = lax.map(route, jnp.arange(PP * M))
    n = TD * TOP
    prio = jnp.argsort(jax.random.uniform(kd[2], (PP * M * EP, n)), axis=-1).astype(jnp.int32)
    r = jax.vmap(ranks)(idx.reshape(PP * M * EP, n), prio).reshape(PP * M, EP, TD, TOP)
    first = (jnp.arange(EP, dtype=jnp.int32) * CG)[None, :, None, None]
    slot = jnp.where(r < CG, r + first, -1).reshape(PP, M, SEQS, L, TOP)
    idx = idx.reshape(PP, M, SEQS, L, TOP)
    g = jax.nn.softmax(1.2 * jax.random.normal(ks[2], (PP, M, SEQS, L, TOP)), axis=-1)
    scale = jnp.exp(0.5 * jax.random.normal(ks[3], (PP, 1, EXPERTS, 1, 1)))
    mu = jax.random.normal(ks[4], (PP, 1, EXPERTS, 1, D))
    O = (scale * (jax.random.normal(ks[5], (PP, M, EXPERTS, C, D)) + 0.8 * mu)).astype(jnp.bfloat16)
    H = jax.random.normal(ks[6], (PP, M, SEQS, L, D)).astype(jnp.bfloat16)
    w = 1.0 + 0.4 * jax.random.normal(kw[0], (PP, D))
    sharp = (0.75 * math.log(L)) ** 0.25 / math.sqrt(D)
    Wq = (sharp * jax.random.normal(kw[1], (PP, D, HEADS, HEAD_DIM))).astype(jnp.bfloat16)
    Wk = (sharp * jax.random.normal(kw[2], (PP, D, HEADS, HEAD_DIM))).astype(jnp.bfloat16)
    Wv = (jax.random.normal(kw[3], (PP, D, HEADS, HEAD_DIM)) / math.sqrt(D)).astype(jnp.bfloat16)
    Wo = (jax.random.normal(kw[4], (PP, HEADS, HEAD_DIM, D)) / math.sqrt(QKV)).astype(jnp.bfloat16)
    return dict(O=O, idx=idx, slot=slot, g=g.astype(jnp.float32), H=H, w=w.astype(jnp.float32), Wq=Wq, Wk=Wk, Wv=Wv, Wo=Wo)


def combine(o, ix, sl, gt, h):
    flat = o.reshape(EXPERTS * C, D)
    acc = h.astype(jnp.float32)
    for kk in range(TOP):
        s = sl[:, kk]
        valid = s >= 0
        rows = jnp.take(flat, ix[:, kk] * C + jnp.where(valid, s, 0), axis=0)
        acc = acc + jnp.where(valid, gt[:, kk], 0.0)[:, None] * rows.astype(jnp.float32)
    return acc.astype(jnp.bfloat16)


def head_attn(a):
    qh, kh, vh = a
    s = jnp.dot(qh, kh.T, preferred_element_type=jnp.float32) * (HEAD_DIM ** -0.5)
    r = lax.broadcasted_iota(jnp.int32, (L, L), 0)
    c = lax.broadcasted_iota(jnp.int32, (L, L), 1)
    p = jax.nn.softmax(jnp.where(r >= c, s, -1e30), axis=-1)
    return jnp.dot(p, vh.astype(jnp.float32))


def layer(y, wn, wq, wk, wv, wo):
    yf = y.astype(jnp.float32)
    x = (yf * lax.rsqrt(jnp.mean(yf * yf, axis=-1, keepdims=True) + EPS) * wn).astype(jnp.bfloat16)
    q = jnp.dot(x, wq.reshape(D, QKV), preferred_element_type=jnp.float32).astype(jnp.bfloat16)
    k = jnp.dot(x, wk.reshape(D, QKV), preferred_element_type=jnp.float32).astype(jnp.bfloat16)
    v = jnp.dot(x, wv.reshape(D, QKV), preferred_element_type=jnp.float32).astype(jnp.bfloat16)

    def heads(t):
        return t.reshape(SEQS, L, HEADS, HEAD_DIM).transpose(0, 2, 1, 3).reshape(SEQS * HEADS, L, HEAD_DIM)

    o = lax.map(head_attn, (heads(q), heads(k), heads(v)))
    o = o.reshape(SEQS, HEADS, L, HEAD_DIM).transpose(0, 2, 1, 3).reshape(T, QKV).astype(jnp.bfloat16)
    a = jnp.dot(o, wo.reshape(QKV, D), preferred_element_type=jnp.float32).astype(jnp.bfloat16)
    return (yf + a.astype(jnp.float32)).astype(jnp.bfloat16)


def reference(O, idx, slot, g, H, w, Wq, Wk, Wv, Wo):
    y = lax.map(lambda a: combine(a[0], a[1], a[2], a[3], a[4]),
                (O.reshape(PP * M, EXPERTS, C, D), idx.reshape(PP * M, T, TOP), slot.reshape(PP * M, T, TOP),
                 g.reshape(PP * M, T, TOP), H.reshape(PP * M, T, D)))
    y = jnp.roll(y.reshape(PP, M, T, D), 1, axis=0)

    def stage(a):
        ys, wn, wq, wk, wv, wo = a
        return lax.map(lambda yy: layer(yy, wn, wq, wk, wv, wo), ys)

    z = lax.map(stage, (y, w, Wq, Wk, Wv, Wo))
    return z.reshape(PP, M, SEQS, L, D)
```

```python
import functools

import jax
import jax.numpy as jnp
from jax import lax
from jax.experimental import pallas as pl
from jax.experimental.pallas import tpu as pltpu
from jax.sharding import PartitionSpec as P

EPS = 1e-6
F32 = jnp.float32
BF16 = jnp.bfloat16
NT = (((1,), (1,)), ((), ()))
VMEM_LIMIT = 60 * 2**20
HS = 4


def gate_terms(pos, gate, g_s, slot):
    t = pos.shape[1]
    rows = g_s.shape[2]
    col = lax.broadcasted_iota(jnp.int32, (t, rows), 1).astype(F32)
    pt = pos.T
    gt = gate.T
    acc = jnp.zeros((t, rows), F32)
    for j in range(pos.shape[0]):
        acc = jnp.where(pt[:, j:j + 1] == col, gt[:, j:j + 1], acc)
    hi = acc.astype(BF16)
    rest = acc - hi.astype(F32)
    mid = rest.astype(BF16)
    g_s[slot, 0:t] = hi
    g_s[slot, t:2 * t] = mid
    g_s[slot, 2 * t:3 * t] = (rest - mid.astype(F32)).astype(BF16)


def front_kernel(sent_ref, here_ref, o_ref, part_ref, *rest):
    n_mb = sent_ref.shape[0]
    far_refs, (near_ref, pg, rows, sums, g_s, own_sem, row_send, row_recv, pg_sem, y_sem, out_sem) = rest[:n_mb - 1], rest[n_mb - 1:]
    n_ep = o_ref.shape[2]
    d = o_ref.shape[-1]
    t = g_s.shape[1] // 3
    e = lax.axis_index('ep')
    mate = e + 1 - 2 * lax.rem(e, 2)
    across = lax.rem(e + 2, n_ep)
    mate_across = lax.rem(mate + 2, n_ep)

    barrier = pltpu.get_barrier_semaphore()
    for dev in (mate, across):
        pl.semaphore_signal(barrier, inc=1, device_id={'ep': dev}, device_id_type=pl.DeviceIdType.MESH)
    pl.semaphore_wait(barrier, 2)

    gates = pltpu.make_async_remote_copy(sent_ref, pg.at[pl.ds(0, n_mb)], pg_sem.at[0], pg_sem.at[1],
                                         device_id={'ep': across}, device_id_type=pl.DeviceIdType.MESH)
    gates.start()
    own, got = [], []
    for i in range(2 * n_mb):
        m = i % n_mb
        mine, theirs = (across, mate_across) if i < n_mb else (e, mate)
        got.append(pltpu.make_async_remote_copy(o_ref.at[m, :, theirs], rows.at[i, 1], row_send.at[i], row_recv.at[i],
                                                device_id={'ep': mate}, device_id_type=pl.DeviceIdType.MESH))
        own.append(pltpu.make_async_copy(o_ref.at[m, :, mine], rows.at[i, 0], own_sem.at[i]))
        got[i].start()
        own[i].start()
    pg[n_mb:] = here_ref[...]
    gates.wait()

    def wait_rows(i):
        pltpu.make_async_copy(o_ref.at[0, :, 0], rows.at[i, 0], own_sem.at[i]).wait()
        pltpu.make_async_remote_copy(o_ref.at[0, :, 0], rows.at[i, 1], row_send.at[i], row_recv.at[i],
                                     device_id={'ep': mate}, device_id_type=pl.DeviceIdType.MESH).wait()

    def gates_of(i):
        gate_terms(pg[i, :8], pg[i, 8:], g_s, lax.rem(i, 2))

    def one(i, _):
        wait_rows(i)
        slot = lax.rem(i, 2)
        gates_of(lax.rem(i + 1, 2 * n_mb))
        for n in range(d // 256):
            c = slice(n * 256, (n + 1) * 256)
            r = jnp.dot(g_s[slot], rows[i, :, :, :, c].reshape(g_s.shape[2], 256), preferred_element_type=F32)
            sums[i, :, c] = (r[2 * t:] + r[t:2 * t]) + r[:t]
        return 0

    gates_of(0)
    one(0, 0)
    first = pltpu.make_async_remote_copy(sums.at[0], part_ref, y_sem.at[0], y_sem.at[1],
                                         device_id={'ep': across}, device_id_type=pl.DeviceIdType.MESH)
    first.start()
    lax.fori_loop(1, n_mb, one, 0)
    outs = [pltpu.make_async_copy(sums.at[m], far_refs[m - 1], out_sem.at[m]) for m in range(1, n_mb)]
    for c in outs:
        c.start()
    lax.fori_loop(n_mb, 2 * n_mb, one, 0)
    near = pltpu.make_async_copy(sums.at[pl.ds(n_mb, n_mb)], near_ref, out_sem.at[0])
    near.start()
    for c in outs + [near]:
        c.wait()
    first.wait()


def front(sent, here, o5):
    mb, ne, nep, cg, d = o5.shape
    t = sent.shape[2]
    one = jax.ShapeDtypeStruct((t, d), F32)
    any_ = pl.BlockSpec(memory_space=pl.ANY)
    vm = pl.BlockSpec(memory_space=pltpu.VMEM)
    dma = pltpu.SemaphoreType.DMA
    return pl.pallas_call(
        front_kernel, name="front",
        in_specs=[vm, vm, any_], out_specs=[any_] * (mb + 1),
        out_shape=[one] * mb + [jax.ShapeDtypeStruct((mb, t, d), F32)],
        scratch_shapes=[pltpu.VMEM((2 * mb,) + sent.shape[1:], F32), pltpu.VMEM((2 * mb, 2, ne, cg, d), BF16),
                        pltpu.VMEM((2 * mb, t, d), F32), pltpu.VMEM((2, 3 * t, 2 * ne * cg), BF16),
                        dma((2 * mb,)), dma((2 * mb,)), dma((2 * mb,)), dma((2,)), dma((2,)), dma((mb,))],
        cost_estimate=pl.CostEstimate(flops=2 * 3 * t * 2 * ne * cg * d * 2 * mb, bytes_accessed=0, transcendentals=0),
        compiler_params=pltpu.CompilerParams(vmem_limit_bytes=VMEM_LIMIT, collective_id=0, has_side_effects=True))(sent, here, o5)


def attn(q, k, v, nb, keep):
    hs = q.shape[1] // 128
    f = 128
    blk = [(h, b) for h in range(hs) for b in range(nb)]

    def cut(t, h, b):
        return t[b * 128:(b + 1) * 128, h * f:(h + 1) * f]

    s = [lax.dot_general(cut(q, h, b), cut(k, h, b), NT, preferred_element_type=F32) for h, b in blk]
    s = [jnp.where(keep, x * (f ** -0.5), -1e30) for x in s]
    m = [jnp.max(x, axis=-1, keepdims=True) for x in s]
    p = [jnp.exp(x - y) for x, y in zip(s, m)]
    d = [jnp.sum(x, axis=-1, keepdims=True) for x in p]
    p = [x * (1.0 / y) for x, y in zip(p, d)]
    o = [jnp.dot(x, cut(v, h, b).astype(F32), preferred_element_type=F32).astype(BF16) for x, (h, b) in zip(p, blk)]
    return jnp.concatenate([jnp.concatenate(o[h * nb:(h + 1) * nb], axis=0) for h in range(hs)], axis=1)


def finish_kernel(h_ref, near_ref, part_ref, out_ref):
    out_ref[...] = (h_ref[...].astype(F32) + near_ref[...] + part_ref[...]).astype(BF16)


def finish(m, h, near, part):
    t, d = part.shape
    one = pl.BlockSpec((None, t // 4, d), lambda i: (m, i, 0))
    flat = pl.BlockSpec((t // 4, d), lambda i: (i, 0))
    return pl.pallas_call(
        finish_kernel, grid=(4,), name="finish", in_specs=[one, one, flat], out_specs=flat,
        out_shape=jax.ShapeDtypeStruct((t, d), BF16),
        cost_estimate=pl.CostEstimate(flops=10**9, bytes_accessed=12 * t * d, transcendentals=0),
        compiler_params=pltpu.CompilerParams(vmem_limit_bytes=VMEM_LIMIT))(h, near, part)


def turn_kernel(c_ref, *refs):
    for i, o in zip(refs[:3], refs[3:]):
        o[...] = jnp.swapaxes(i[...], 0, 1)


def turn(core, ws):
    d, nh, f = ws[0].shape
    hc, kb = nh // 2, 256
    return pl.pallas_call(
        turn_kernel, name="turn",
        grid_spec=pltpu.PrefetchScalarGridSpec(
            num_scalar_prefetch=1, grid=(d // kb,),
            in_specs=[pl.BlockSpec((kb, hc, f), lambda i, c: (i, c[0], 0))] * 3,
            out_specs=[pl.BlockSpec((hc, kb, f), lambda i, c: (0, i, 0))] * 3),
        out_shape=[jax.ShapeDtypeStruct((hc, d, f), BF16)] * 3,
        cost_estimate=pl.CostEstimate(flops=10**10, bytes_accessed=6 * d * hc * f * 2, transcendentals=0),
        compiler_params=pltpu.CompilerParams(vmem_limit_bytes=VMEM_LIMIT))(core, *ws)


def layer_kernel(c_ref, u_ref, v_ref, w_ref, q_ref, k_ref, vw_ref, o_ref, mine_ref, mate_ref, x_s):
    step = pl.program_id(0)
    half, d = u_ref.shape
    nb = 2 * half // 128

    @pl.when(step == 0)
    def _():
        for j, r_ref in enumerate((u_ref, v_ref)):
            for b in range(half // 128):
                uf = r_ref[b * 128:(b + 1) * 128].astype(F32)
                r = lax.rsqrt(jnp.mean(uf * uf, axis=-1, keepdims=True) + EPS)
                x_s[j * half + b * 128:j * half + (b + 1) * 128] = (uf * r * w_ref[...]).astype(BF16)

    keep = lax.broadcasted_iota(jnp.int32, (128, 128), 0) >= lax.broadcasted_iota(jnp.int32, (128, 128), 1)

    def proj(ref):
        wt = jnp.concatenate([ref[i] for i in range(ref.shape[0])], axis=1)
        return jnp.dot(x_s[...], wt, preferred_element_type=F32).astype(BF16)

    q, k, v = proj(q_ref), proj(k_ref), proj(vw_ref)
    a = attn(q, k, v, nb, keep)
    t = jnp.dot(a, o_ref[...].reshape(a.shape[1], d), preferred_element_type=F32)

    @pl.when(step == 0)
    def _():
        mine_ref[...] = t[:half]
        mate_ref[...] = t[half:]

    @pl.when(step > 0)
    def _():
        mine_ref[...] += t[:half]
        mate_ref[...] += t[half:]


def layer(core, u, v, w, wq, wk, wv, wo):
    m, d = u.shape
    hc, _, f = wq.shape
    wspec = pl.BlockSpec((HS, d, f), lambda i, c: (i, 0, 0))
    full = pl.BlockSpec((m, d), lambda i, c: (0, 0))
    return pl.pallas_call(
        layer_kernel, name="layer",
        grid_spec=pltpu.PrefetchScalarGridSpec(
            num_scalar_prefetch=1, grid=(hc // HS,),
            in_specs=[full, full, pl.BlockSpec((1, d), lambda i, c: (0, 0)), wspec, wspec, wspec,
                      pl.BlockSpec((HS, f, d), lambda i, c: (c[0] * (hc // HS) + i, 0, 0))],
            out_specs=[full, full],
            scratch_shapes=[pltpu.VMEM((2 * m, d), BF16)]),
        out_shape=[jax.ShapeDtypeStruct((m, d), F32)] * 2,
        cost_estimate=pl.CostEstimate(flops=2 * 2 * m * d * hc * f * 4 * 2, bytes_accessed=4 * d * hc * f * 2, transcendentals=0),
        compiler_params=pltpu.CompilerParams(vmem_limit_bytes=VMEM_LIMIT))(core, u, v, w, wq, wk, wv, wo)


def solution(mesh):
    npp = mesh.shape['pp']
    nep = mesh.shape['ep']
    perm = [(i, (i + 1) % npp) for i in range(npp)]
    mate = [(i, i ^ 1) for i in range(nep)]
    across = [(i, i ^ 2) for i in range(nep)]
    tok = P(('data', 'pp'), None, 'ep', None, None)
    wsp = P('pp', None, None, None)

    def body(O, idx, slot, g, H, w, Wq, Wk, Wv, Wo):
        o = O[0]
        mb, ne, cap, d = o.shape
        cg = cap // nep
        o5 = o.reshape(mb, ne, nep, cg, d)
        e = lax.axis_index('ep')
        core = e % 2
        ix, sl, gt = (jnp.swapaxes(a[0][:, 0], 1, 2) for a in (idx, slot, g))

        def place(chip, reader):
            k = ix - chip * (2 * ne)
            ok = (sl >= 0) & (k >= 0) & (k < 2 * ne)
            k = jnp.where(reader == 0, k, (k + ne) % (2 * ne))
            return jnp.where(ok, k * cg + sl - e * cg, -1).astype(F32)

        here = place(e // 2, core)
        sent = jnp.concatenate([place(1 - e // 2, core), gt], axis=1)
        part0, *far, near = front(sent, jnp.concatenate([here, gt], axis=1), o5)
        part = [part0] + [lax.ppermute(x, 'ep', across) for x in far]
        cs = jnp.reshape(core, (1,)).astype(jnp.int32)
        h = H[0][:, 0]
        z = [None] * mb

        def tail(m, u):
            mine, other = layer(cs, u, lax.ppermute(u, 'ep', mate), w, *wt, Wo[0])
            other = lax.ppermute(other, 'ep', mate)
            z[m] = (u, mine, other)
            return mine

        y = finish(0, h, near, part[0])
        ws, y, near = lax.optimization_barrier(((Wq[0], Wk[0], Wv[0]), y, near))
        late = lax.ppermute(y, 'pp', perm)
        wt = turn(cs, ws)
        wt, near = lax.optimization_barrier((wt, near))
        for m in range(1, mb):
            y = finish(m, h, near, part[m])
            late, y = lax.optimization_barrier((late, y))
            u = lax.ppermute(y, 'pp', perm)
            mine = tail(m - 1, late)
            mine, near = lax.optimization_barrier((mine, near))
            late = u
        tail(mb - 1, late)
        z = [(u.astype(F32) + (mine + other).astype(BF16).astype(F32)).astype(BF16) for u, mine, other in z]
        return jnp.stack(z).reshape(1, mb, 1, H.shape[3], d)

    return jax.shard_map(body, mesh=mesh,
                         in_specs=(tok, tok, tok, tok, tok, P('pp', None), wsp, wsp, wsp, wsp),
                         out_specs=tok, check_vma=False)
```

```python
import jax
import jax.numpy as jnp
from jax import lax
from jax.experimental import pallas as pl
from jax.experimental.pallas import tpu as pltpu
from jax.sharding import PartitionSpec as P


EPS = 1e-6
F32 = jnp.float32
BF16 = jnp.bfloat16
NT = (((1,), (1,)), ((), ()))
VMEM_LIMIT = 60 * 2**20
HS = 4


def gate_terms(pos, gate, g_s, slot):
    t = pos.shape[1]
    rows = g_s.shape[2]
    col = lax.broadcasted_iota(jnp.int32, (t, rows), 1).astype(F32)
    pt = pos.T
    gt = gate.T
    acc = jnp.zeros((t, rows), F32)
    for j in range(pos.shape[0]):
        acc = jnp.where(pt[:, j:j + 1] == col, gt[:, j:j + 1], acc)
    hi = acc.astype(BF16)
    rest = acc - hi.astype(F32)
    mid = rest.astype(BF16)
    g_s[slot, 0:t] = hi
    g_s[slot, t:2 * t] = mid
    g_s[slot, 2 * t:3 * t] = (rest - mid.astype(F32)).astype(BF16)


def front_kernel(sent_ref, here_ref, o_ref, part_ref, *rest):
    n_mb = sent_ref.shape[0]
    far_refs, (near_ref, pg, rows, sums, g_s, own_sem, row_send, row_recv, pg_sem, y_sem, out_sem) = rest[:n_mb - 1], rest[n_mb - 1:]
    n_ep = o_ref.shape[2]
    d = o_ref.shape[-1]
    t = g_s.shape[1] // 3
    e = lax.axis_index('ep')
    mate = e + 1 - 2 * lax.rem(e, 2)
    across = lax.rem(e + 2, n_ep)
    mate_across = lax.rem(mate + 2, n_ep)

    barrier = pltpu.get_barrier_semaphore()
    for dev in (mate, across):
        pl.semaphore_signal(barrier, inc=1, device_id={'ep': dev}, device_id_type=pl.DeviceIdType.MESH)
    pl.semaphore_wait(barrier, 2)

    gates = pltpu.make_async_remote_copy(sent_ref, pg.at[pl.ds(0, n_mb)], pg_sem.at[0], pg_sem.at[1],
                                         device_id={'ep': across}, device_id_type=pl.DeviceIdType.MESH)
    gates.start()
    own, got = [], []
    for i in range(2 * n_mb):
        m = i % n_mb
        mine, theirs = (across, mate_across) if i < n_mb else (e, mate)
        got.append(pltpu.make_async_remote_copy(o_ref.at[m, :, theirs], rows.at[i, 1], row_send.at[i], row_recv.at[i],
                                                device_id={'ep': mate}, device_id_type=pl.DeviceIdType.MESH))
        own.append(pltpu.make_async_copy(o_ref.at[m, :, mine], rows.at[i, 0], own_sem.at[i]))
        got[i].start()
        own[i].start()
    pg[n_mb:] = here_ref[...]
    gates.wait()

    def wait_rows(i):
        pltpu.make_async_copy(o_ref.at[0, :, 0], rows.at[i, 0], own_sem.at[i]).wait()
        pltpu.make_async_remote_copy(o_ref.at[0, :, 0], rows.at[i, 1], row_send.at[i], row_recv.at[i],
                                     device_id={'ep': mate}, device_id_type=pl.DeviceIdType.MESH).wait()

    def gates_of(i):
        gate_terms(pg[i, :8], pg[i, 8:], g_s, lax.rem(i, 2))

    def one(i, _):
        wait_rows(i)
        slot = lax.rem(i, 2)
        gates_of(lax.rem(i + 1, 2 * n_mb))
        for n in range(d // 256):
            c = slice(n * 256, (n + 1) * 256)
            r = jnp.dot(g_s[slot], rows[i, :, :, :, c].reshape(g_s.shape[2], 256), preferred_element_type=F32)
            sums[i, :, c] = (r[2 * t:] + r[t:2 * t]) + r[:t]
        return 0

    gates_of(0)
    one(0, 0)
    first = pltpu.make_async_remote_copy(sums.at[0], part_ref, y_sem.at[0], y_sem.at[1],
                                         device_id={'ep': across}, device_id_type=pl.DeviceIdType.MESH)
    first.start()
    lax.fori_loop(1, n_mb, one, 0)
    outs = [pltpu.make_async_copy(sums.at[m], far_refs[m - 1], out_sem.at[m]) for m in range(1, n_mb)]
    for c in outs:
        c.start()
    lax.fori_loop(n_mb, 2 * n_mb, one, 0)
    near = pltpu.make_async_copy(sums.at[pl.ds(n_mb, n_mb)], near_ref, out_sem.at[0])
    near.start()
    for c in outs + [near]:
        c.wait()
    first.wait()


def front(sent, here, o5):
    mb, ne, _, cg, d = o5.shape
    t = sent.shape[2]
    one = jax.ShapeDtypeStruct((t, d), F32)
    any_ = pl.BlockSpec(memory_space=pl.ANY)
    vm = pl.BlockSpec(memory_space=pltpu.VMEM)
    dma = pltpu.SemaphoreType.DMA
    return pl.pallas_call(
        front_kernel, name="front",
        in_specs=[vm, vm, any_], out_specs=[any_] * (mb + 1),
        out_shape=[one] * mb + [jax.ShapeDtypeStruct((mb, t, d), F32)],
        scratch_shapes=[pltpu.VMEM((2 * mb,) + sent.shape[1:], F32), pltpu.VMEM((2 * mb, 2, ne, cg, d), BF16),
                        pltpu.VMEM((2 * mb, t, d), F32), pltpu.VMEM((2, 3 * t, 2 * ne * cg), BF16),
                        dma((2 * mb,)), dma((2 * mb,)), dma((2 * mb,)), dma((2,)), dma((2,)), dma((mb,))],
        cost_estimate=pl.CostEstimate(flops=2 * 3 * t * 2 * ne * cg * d * 2 * mb, bytes_accessed=0, transcendentals=0),
        compiler_params=pltpu.CompilerParams(vmem_limit_bytes=VMEM_LIMIT, collective_id=0, has_side_effects=True))(sent, here, o5)


def attn(q, k, v, nb, keep):
    hs = q.shape[1] // 128
    f = 128
    blk = [(h, b) for h in range(hs) for b in range(nb)]

    def cut(t, h, b):
        return t[b * 128:(b + 1) * 128, h * f:(h + 1) * f]

    s = [lax.dot_general(cut(q, h, b), cut(k, h, b), NT, preferred_element_type=F32) for h, b in blk]
    s = [jnp.where(keep, x * (f ** -0.5), -1e30) for x in s]
    m = [jnp.max(x, axis=-1, keepdims=True) for x in s]
    p = [jnp.exp(x - y) for x, y in zip(s, m)]
    d = [jnp.sum(x, axis=-1, keepdims=True) for x in p]
    p = [x * (1.0 / y) for x, y in zip(p, d)]
    o = [jnp.dot(x, cut(v, h, b).astype(F32), preferred_element_type=F32).astype(BF16) for x, (h, b) in zip(p, blk)]
    return jnp.concatenate([jnp.concatenate(o[h * nb:(h + 1) * nb], axis=0) for h in range(hs)], axis=1)


def turn_kernel(c_ref, q_ref, k_ref, v_ref, o_ref, qt_ref, kt_ref, vt_ref, ot_ref, sem):
    step = pl.program_id(0)
    hc = ot_ref.shape[0]
    kb = q_ref.shape[0]
    copy = pltpu.make_async_copy(o_ref.at[pl.ds(c_ref[0] * hc, hc)], ot_ref, sem)

    @pl.when(step == 0)
    def _():
        copy.start()

    rows = pl.ds(pl.multiple_of(step * kb, kb), kb)
    for i, o in ((q_ref, qt_ref), (k_ref, kt_ref), (v_ref, vt_ref)):
        o[:, rows, :] = jnp.swapaxes(i[...], 0, 1)

    @pl.when(step == pl.num_programs(0) - 1)
    def _():
        copy.wait()


def turn(core, wq, wk, wv, wo):
    d, nh, f = wq.shape
    hc, kb = nh // 2, 128
    vm = pl.BlockSpec(memory_space=pltpu.VMEM)
    return pl.pallas_call(
        turn_kernel, name="turn",
        grid_spec=pltpu.PrefetchScalarGridSpec(
            num_scalar_prefetch=1, grid=(d // kb,),
            in_specs=[pl.BlockSpec((kb, hc, f), lambda i, c: (i, c[0], 0))] * 3 + [pl.BlockSpec(memory_space=pl.ANY)],
            out_specs=[vm] * 4, scratch_shapes=[pltpu.SemaphoreType.DMA]),
        out_shape=[jax.ShapeDtypeStruct((hc, d, f), BF16)] * 3 + [jax.ShapeDtypeStruct((hc, f, d), BF16)],
        cost_estimate=pl.CostEstimate(flops=10**10, bytes_accessed=4 * d * hc * f * 2, transcendentals=0),
        compiler_params=pltpu.CompilerParams(vmem_limit_bytes=16 * 2**20))(core, wq, wk, wv, wo)


def layer_kernel(u_ref, v_ref, w_ref, q_ref, k_ref, vw_ref, o_ref, mine_ref, mate_ref, x_s):
    half, d = u_ref.shape
    hc = q_ref.shape[0]
    nb = 2 * half // 128
    for j, r_ref in enumerate((u_ref, v_ref)):
        for b in range(half // 128):
            uf = r_ref[b * 128:(b + 1) * 128].astype(F32)
            r = lax.rsqrt(jnp.mean(uf * uf, axis=-1, keepdims=True) + EPS)
            x_s[j * half + b * 128:j * half + (b + 1) * 128] = (uf * r * w_ref[...]).astype(BF16)
    keep = lax.broadcasted_iota(jnp.int32, (128, 128), 0) >= lax.broadcasted_iota(jnp.int32, (128, 128), 1)

    def heads(i):
        at = i * HS

        def proj(ref):
            wt = jnp.concatenate([ref[at + j] for j in range(HS)], axis=1)
            return jnp.dot(x_s[...], wt, preferred_element_type=F32).astype(BF16)

        q, k, v = proj(q_ref), proj(k_ref), proj(vw_ref)
        a = attn(q, k, v, nb, keep)
        return jnp.dot(a, o_ref[pl.ds(at, HS)].reshape(a.shape[1], d), preferred_element_type=F32)

    t = heads(0)
    mine_ref[...] = t[:half]
    mate_ref[...] = t[half:]

    def more(i, _):
        t = heads(i)
        mine_ref[...] += t[:half]
        mate_ref[...] += t[half:]
        return 0

    lax.fori_loop(1, hc // HS, more, 0)


def layer(u, v, w, wq, wk, wv, wo):
    m, d = u.shape
    hc, _, f = wq.shape
    vm = pl.BlockSpec(memory_space=pltpu.VMEM)
    return pl.pallas_call(
        layer_kernel, name="layer", in_specs=[vm] * 7, out_specs=[vm] * 2,
        scratch_shapes=[pltpu.VMEM((2 * m, d), BF16)],
        out_shape=[jax.ShapeDtypeStruct((m, d), F32)] * 2,
        cost_estimate=pl.CostEstimate(flops=2 * 2 * m * d * hc * f * 4 * 2, bytes_accessed=4 * d * hc * f * 2, transcendentals=0),
        compiler_params=pltpu.CompilerParams(vmem_limit_bytes=20 * 2**20))(u, v, w, wq, wk, wv, wo)


def solution(mesh):
    npp = mesh.shape['pp']
    nep = mesh.shape['ep']
    perm = [(i, (i + 1) % npp) for i in range(npp)]
    mate = [(i, i ^ 1) for i in range(nep)]
    across = [(i, i ^ 2) for i in range(nep)]
    tok = P(('data', 'pp'), None, 'ep', None, None)
    wsp = P('pp', None, None, None)

    def step(O, idx, slot, g, H, w, Wq, Wk, Wv, Wo):
        o = O[0]
        mb, ne, cap, d = o.shape
        cg = cap // nep
        o5 = o.reshape(mb, ne, nep, cg, d)
        e = lax.axis_index('ep')
        core = e % 2
        ix, sl, gt = (jnp.swapaxes(a[0][:, 0], 1, 2) for a in (idx, slot, g))

        def place(chip, reader):
            k = ix - chip * (2 * ne)
            ok = (sl >= 0) & (k >= 0) & (k < 2 * ne)
            k = jnp.where(reader == 0, k, (k + ne) % (2 * ne))
            return jnp.where(ok, k * cg + sl - e * cg, -1).astype(F32)

        here = place(e // 2, core)
        sent = jnp.concatenate([place(1 - e // 2, core), gt], axis=1)
        part0, *far, near = front(sent, jnp.concatenate([here, gt], axis=1), o5)
        part = [part0]
        for m in range(1, mb):
            part.append(lax.ppermute(far[m - 1], 'ep', across))
        cs = jnp.reshape(core, (1,)).astype(jnp.int32)
        h = H[0][:, 0]
        z = [None] * mb

        def finish(m, near):
            return (h[m].astype(F32) + near[m] + part[m]).astype(BF16)

        def start(u):
            mine, other = layer(u, lax.ppermute(u, 'ep', mate), w, *wt)
            return u, mine, lax.ppermute(other, 'ep', mate)

        def end(u, mine, other):
            return (u.astype(F32) + (mine + other).astype(BF16).astype(F32)).astype(BF16)

        y = finish(0, near)
        ws, y, near = lax.optimization_barrier(((Wq[0], Wk[0], Wv[0], Wo[0]), y, near))
        late = lax.ppermute(y, 'pp', perm)
        wt = turn(cs, *ws)
        wt, near = lax.optimization_barrier((wt, near))
        for m in range(1, mb):
            y = finish(m, near)
            late, y = lax.optimization_barrier((late, y))
            u = lax.ppermute(y, 'pp', perm)
            last = start(late)
            z[m - 1] = last
            mine, near = lax.optimization_barrier((last[1], near))
            z[m - 1] = (last[0], mine, last[2])
            late = u
        z[mb - 1] = start(late)
        z = [end(*q) for q in z]
        return jnp.stack(z).reshape(1, mb, 1, H.shape[3], d)

    return jax.shard_map(step, mesh=mesh,
                         in_specs=(tok, tok, tok, tok, tok, P('pp', None), wsp, wsp, wsp, wsp),
                         out_specs=tok, check_vma=False)
```

```python
import jax
import jax.numpy as jnp
from jax import lax
from jax.experimental import pallas as pl
from jax.experimental.pallas import tpu as pltpu
from jax.sharding import PartitionSpec as P


EPS = 1e-6
F32 = jnp.float32
BF16 = jnp.bfloat16
NT = (((1,), (1,)), ((), ()))
VMEM_LIMIT = 60 * 2**20
HS = 4
IN_FRONT = 2


def gate_terms(pos, gate, g_s, slot):
    t = pos.shape[1]
    rows = g_s.shape[2]
    col = lax.broadcasted_iota(jnp.int32, (t, rows), 1).astype(F32)
    pt = pos.T
    gt = gate.T
    acc = jnp.zeros((t, rows), F32)
    for j in range(pos.shape[0]):
        acc = jnp.where(pt[:, j:j + 1] == col, gt[:, j:j + 1], acc)
    hi = acc.astype(BF16)
    rest = acc - hi.astype(F32)
    mid = rest.astype(BF16)
    g_s[slot, 0:t] = hi
    g_s[slot, t:2 * t] = mid
    g_s[slot, 2 * t:3 * t] = (rest - mid.astype(F32)).astype(BF16)


def place(ix, sl, chip, core, e, ne, cg):
    k = ix - chip * (2 * ne)
    ok = (sl >= 0) & (k >= 0) & (k < 2 * ne)
    k = jnp.where(k >= ne, k - ne, k + ne) * core + k * (1 - core)
    return jnp.where(ok, k * cg + sl - e * cg, -1).astype(F32)


def front_kernel(ix_ref, sl_ref, gt_ref, o_ref, *rest):
    n_mb, ne, n_ep, cg, d = o_ref.shape
    in_refs, far_refs = rest[:IN_FRONT], rest[IN_FRONT:n_mb]
    near_ref, sent, pg, rows, sums, g_s, own_sem, row_send, row_recv, pg_sem, y_send, y_recv, out_sem = rest[n_mb:]
    t = g_s.shape[1] // 3
    e = lax.axis_index('ep')
    core = lax.rem(e, 2)
    chip = e // 2
    mate = e + 1 - 2 * core
    across = lax.rem(e + 2, n_ep)
    mate_across = lax.rem(mate + 2, n_ep)

    sent[:, :8] = place(ix_ref[...], sl_ref[...], 1 - chip, core, e, ne, cg)
    sent[:, 8:] = gt_ref[...]
    barrier = pltpu.get_barrier_semaphore()
    for dev in (mate, across):
        pl.semaphore_signal(barrier, inc=1, device_id={'ep': dev}, device_id_type=pl.DeviceIdType.MESH)
    pl.semaphore_wait(barrier, 2)

    gates = pltpu.make_async_remote_copy(sent, pg.at[pl.ds(0, n_mb)], pg_sem.at[0], pg_sem.at[1],
                                         device_id={'ep': across}, device_id_type=pl.DeviceIdType.MESH)
    gates.start()
    own, got = [], []
    for i in range(2 * n_mb):
        m = i % n_mb
        mine, theirs = (across, mate_across) if i < n_mb else (e, mate)
        got.append(pltpu.make_async_remote_copy(o_ref.at[m, :, theirs], rows.at[i, 1], row_send.at[i], row_recv.at[i],
                                                device_id={'ep': mate}, device_id_type=pl.DeviceIdType.MESH))
        own.append(pltpu.make_async_copy(o_ref.at[m, :, mine], rows.at[i, 0], own_sem.at[i]))
        got[i].start()
        own[i].start()
    pg[n_mb:, :8] = place(ix_ref[...], sl_ref[...], chip, core, e, ne, cg)
    pg[n_mb:, 8:] = gt_ref[...]
    gates.wait()

    def wait_rows(i):
        pltpu.make_async_copy(o_ref.at[0, :, 0], rows.at[i, 0], own_sem.at[i]).wait()
        pltpu.make_async_remote_copy(o_ref.at[0, :, 0], rows.at[i, 1], row_send.at[i], row_recv.at[i],
                                     device_id={'ep': mate}, device_id_type=pl.DeviceIdType.MESH).wait()

    def gates_of(i):
        gate_terms(pg[i, :8], pg[i, 8:], g_s, lax.rem(i, 2))

    def one(i, _):
        wait_rows(i)
        slot = lax.rem(i, 2)
        gates_of(lax.rem(i + 1, 2 * n_mb))
        for n in range(d // 256):
            c = slice(n * 256, (n + 1) * 256)
            r = jnp.dot(g_s[slot], rows[i, :, :, :, c].reshape(g_s.shape[2], 256), preferred_element_type=F32)
            sums[i, :, c] = (r[2 * t:] + r[t:2 * t]) + r[:t]
        return 0

    gates_of(0)
    first = []
    for i in range(IN_FRONT):
        one(i, 0)
        first.append(pltpu.make_async_remote_copy(sums.at[i], in_refs[i], y_send.at[i], y_recv.at[i],
                                                  device_id={'ep': across}, device_id_type=pl.DeviceIdType.MESH))
        first[i].start()
    lax.fori_loop(IN_FRONT, n_mb, one, 0)
    outs = [pltpu.make_async_copy(sums.at[m], far_refs[m - IN_FRONT], out_sem.at[m]) for m in range(IN_FRONT, n_mb)]
    for c in outs:
        c.start()
    lax.fori_loop(n_mb, 2 * n_mb, one, 0)
    near = pltpu.make_async_copy(sums.at[pl.ds(n_mb, n_mb)], near_ref, out_sem.at[0])
    near.start()
    for c in outs + [near] + first:
        c.wait()


def front(ix, sl, gt, o5):
    mb, ne, _, cg, d = o5.shape
    t = ix.shape[2]
    one = jax.ShapeDtypeStruct((t, d), F32)
    any_ = pl.BlockSpec(memory_space=pl.ANY)
    vm = pl.BlockSpec(memory_space=pltpu.VMEM)
    dma = pltpu.SemaphoreType.DMA
    return pl.pallas_call(
        front_kernel, name="front",
        in_specs=[vm, vm, vm, any_], out_specs=[any_] * (mb + 1),
        out_shape=[one] * mb + [jax.ShapeDtypeStruct((mb, t, d), F32)],
        scratch_shapes=[pltpu.VMEM((mb, 16, t), F32), pltpu.VMEM((2 * mb, 16, t), F32), pltpu.VMEM((2 * mb, 2, ne, cg, d), BF16),
                        pltpu.VMEM((2 * mb, t, d), F32), pltpu.VMEM((2, 3 * t, 2 * ne * cg), BF16),
                        dma((2 * mb,)), dma((2 * mb,)), dma((2 * mb,)), dma((2,)), dma((IN_FRONT,)), dma((IN_FRONT,)), dma((mb,))],
        cost_estimate=pl.CostEstimate(flops=2 * 3 * t * 2 * ne * cg * d * 2 * mb, bytes_accessed=0, transcendentals=0),
        compiler_params=pltpu.CompilerParams(vmem_limit_bytes=VMEM_LIMIT, collective_id=0, has_side_effects=True))(ix, sl, gt, o5)


def attn(q, k, v, nb, keep):
    hs = q.shape[1] // 128
    f = 128
    blk = [(h, b) for h in range(hs) for b in range(nb)]

    def cut(t, h, b):
        return t[b * 128:(b + 1) * 128, h * f:(h + 1) * f]

    s = [lax.dot_general(cut(q, h, b), cut(k, h, b), NT, preferred_element_type=F32) for h, b in blk]
    s = [jnp.where(keep, x * (f ** -0.5), -1e30) for x in s]
    m = [jnp.max(x, axis=-1, keepdims=True) for x in s]
    p = [jnp.exp(x - y) for x, y in zip(s, m)]
    d = [jnp.sum(x, axis=-1, keepdims=True) for x in p]
    p = [x * (1.0 / y) for x, y in zip(p, d)]
    o = [jnp.dot(x, cut(v, h, b).astype(F32), preferred_element_type=F32).astype(BF16) for x, (h, b) in zip(p, blk)]
    return jnp.concatenate([jnp.concatenate(o[h * nb:(h + 1) * nb], axis=0) for h in range(hs)], axis=1)


def turn_kernel(c_ref, q_ref, k_ref, v_ref, o_ref, qt_ref, kt_ref, vt_ref, ot_ref, sem):
    step = pl.program_id(0)
    hc = ot_ref.shape[0]
    kb = q_ref.shape[0]
    copy = pltpu.make_async_copy(o_ref.at[pl.ds(c_ref[0] * hc, hc)], ot_ref, sem)

    @pl.when(step == 0)
    def _():
        copy.start()

    rows = pl.ds(pl.multiple_of(step * kb, kb), kb)
    for i, o in ((q_ref, qt_ref), (k_ref, kt_ref), (v_ref, vt_ref)):
        o[:, rows, :] = jnp.swapaxes(i[...], 0, 1)

    @pl.when(step == pl.num_programs(0) - 1)
    def _():
        copy.wait()


def turn(core, wq, wk, wv, wo):
    d, nh, f = wq.shape
    hc, kb = nh // 2, 128
    vm = pl.BlockSpec(memory_space=pltpu.VMEM)
    return pl.pallas_call(
        turn_kernel, name="turn",
        grid_spec=pltpu.PrefetchScalarGridSpec(
            num_scalar_prefetch=1, grid=(d // kb,),
            in_specs=[pl.BlockSpec((kb, hc, f), lambda i, c: (i, c[0], 0))] * 3 + [pl.BlockSpec(memory_space=pl.ANY)],
            out_specs=[vm] * 4, scratch_shapes=[pltpu.SemaphoreType.DMA]),
        out_shape=[jax.ShapeDtypeStruct((hc, d, f), BF16)] * 3 + [jax.ShapeDtypeStruct((hc, f, d), BF16)],
        cost_estimate=pl.CostEstimate(flops=10**10, bytes_accessed=4 * d * hc * f * 2, transcendentals=0),
        compiler_params=pltpu.CompilerParams(vmem_limit_bytes=16 * 2**20))(core, wq, wk, wv, wo)


def layer_kernel(u_ref, v_ref, w_ref, q_ref, k_ref, vw_ref, o_ref, mine_ref, mate_ref, x_s):
    half, d = u_ref.shape
    hc = q_ref.shape[0]
    nb = 2 * half // 128
    for j, r_ref in enumerate((u_ref, v_ref)):
        for b in range(half // 128):
            uf = r_ref[b * 128:(b + 1) * 128].astype(F32)
            r = lax.rsqrt(jnp.mean(uf * uf, axis=-1, keepdims=True) + EPS)
            x_s[j * half + b * 128:j * half + (b + 1) * 128] = (uf * r * w_ref[...]).astype(BF16)
    keep = lax.broadcasted_iota(jnp.int32, (128, 128), 0) >= lax.broadcasted_iota(jnp.int32, (128, 128), 1)

    def heads(i):
        at = i * HS

        def proj(ref):
            wt = jnp.concatenate([ref[at + j] for j in range(HS)], axis=1)
            return jnp.dot(x_s[...], wt, preferred_element_type=F32).astype(BF16)

        q, k, v = proj(q_ref), proj(k_ref), proj(vw_ref)
        a = attn(q, k, v, nb, keep)
        return jnp.dot(a, o_ref[pl.ds(at, HS)].reshape(a.shape[1], d), preferred_element_type=F32)

    mine_ref[...] = jnp.zeros_like(mine_ref)
    mate_ref[...] = jnp.zeros_like(mate_ref)

    def more(i, _):
        t = heads(i)
        mine_ref[...] += t[:half]
        mate_ref[...] += t[half:]
        return 0

    lax.fori_loop(0, hc // HS, more, 0)


def layer(u, v, w, wq, wk, wv, wo):
    m, d = u.shape
    hc, _, f = wq.shape
    vm = pl.BlockSpec(memory_space=pltpu.VMEM)
    return pl.pallas_call(
        layer_kernel, name="layer", in_specs=[vm] * 7, out_specs=[vm] * 2,
        scratch_shapes=[pltpu.VMEM((2 * m, d), BF16)],
        out_shape=[jax.ShapeDtypeStruct((m, d), F32)] * 2,
        cost_estimate=pl.CostEstimate(flops=2 * 2 * m * d * hc * f * 4 * 2, bytes_accessed=4 * d * hc * f * 2, transcendentals=0),
        compiler_params=pltpu.CompilerParams(vmem_limit_bytes=12 * 2**20))(u, v, w, wq, wk, wv, wo)


def solution(mesh):
    npp = mesh.shape['pp']
    nep = mesh.shape['ep']
    perm = [(i, (i + 1) % npp) for i in range(npp)]
    mate = [(i, i ^ 1) for i in range(nep)]
    across = [(i, i ^ 2) for i in range(nep)]
    tok = P(('data', 'pp'), None, 'ep', None, None)
    wsp = P('pp', None, None, None)

    def step(O, idx, slot, g, H, w, Wq, Wk, Wv, Wo):
        o = O[0]
        mb, ne, cap, d = o.shape
        cg = cap // nep
        o5 = o.reshape(mb, ne, nep, cg, d)
        e = lax.axis_index('ep')
        core = e % 2
        ix, sl, gt = (jnp.swapaxes(a[0][:, 0], 1, 2) for a in (idx, slot, g))

        *part, near = front(ix, sl, gt, o5)
        for m in range(IN_FRONT, mb):
            part[m] = lax.ppermute(part[m], 'ep', across)
        cs = jnp.reshape(core, (1,)).astype(jnp.int32)
        h = H[0][:, 0]
        z = [None] * mb

        def finish(m, near):
            return (h[m].astype(F32) + near[m] + part[m]).astype(BF16)

        def start(u):
            mine, other = layer(u, lax.ppermute(u, 'ep', mate), w, *wt)
            return u, mine, lax.ppermute(other, 'ep', mate)

        def end(u, mine, other):
            return (u.astype(F32) + (mine + other).astype(BF16).astype(F32)).astype(BF16)

        y = [finish(m, near) for m in range(IN_FRONT)]
        ws, y, near = lax.optimization_barrier(((Wq[0], Wk[0], Wv[0], Wo[0]), y, near))
        u = [lax.ppermute(x, 'pp', perm) for x in y]
        wt = turn(cs, *ws)
        wt, near = lax.optimization_barrier((wt, near))
        for m in range(IN_FRONT, mb + IN_FRONT):
            k = m - IN_FRONT
            late = u[k]
            if m < mb:
                y = finish(m, near)
                late, y = lax.optimization_barrier((late, y))
                u.append(lax.ppermute(y, 'pp', perm))
            z[k] = start(late)
            mine, near = lax.optimization_barrier((z[k][1], near))
            z[k] = (z[k][0], mine, z[k][2])
            if k > 0:
                prev, mine = lax.optimization_barrier((z[k - 1], mine))
                z[k - 1] = end(*prev)
                z[k] = (z[k][0], mine, z[k][2])
        z[mb - 1] = end(*z[mb - 1])
        return jnp.stack(z).reshape(1, mb, 1, H.shape[3], d)

    return jax.shard_map(step, mesh=mesh,
                         in_specs=(tok, tok, tok, tok, tok, P('pp', None), wsp, wsp, wsp, wsp),
                         out_specs=tok, check_vma=False)
```

```python
import jax
import jax.numpy as jnp
from jax import lax
from jax.experimental import pallas as pl
from jax.experimental.pallas import tpu as pltpu
from jax.sharding import PartitionSpec as P


EPS = 1e-6
F32 = jnp.float32
BF16 = jnp.bfloat16
NT = (((1,), (1,)), ((), ()))
VMEM_LIMIT = 60 * 2**20
HS = 4
IN_FRONT = 1


def gate_terms(pos, gate, g_s, slot):
    t = pos.shape[1]
    rows = g_s.shape[2]
    col = lax.broadcasted_iota(jnp.int32, (t, rows), 1).astype(F32)
    pt = pos.T
    gt = gate.T
    acc = jnp.zeros((t, rows), F32)
    for j in range(pos.shape[0]):
        acc = jnp.where(pt[:, j:j + 1] == col, gt[:, j:j + 1], acc)
    hi = acc.astype(BF16)
    rest = acc - hi.astype(F32)
    mid = rest.astype(BF16)
    g_s[slot, 0:t] = hi
    g_s[slot, t:2 * t] = mid
    g_s[slot, 2 * t:3 * t] = (rest - mid.astype(F32)).astype(BF16)


def place(ix, sl, chip, core, e, ne, cg):
    k = ix - chip * (2 * ne)
    ok = (sl >= 0) & (k >= 0) & (k < 2 * ne)
    k = jnp.where(k >= ne, k - ne, k + ne) * core + k * (1 - core)
    return jnp.where(ok, k * cg + sl - e * cg, -1).astype(F32)


def front_kernel(ix_ref, sl_ref, gt_ref, o_ref, *rest):
    n_mb, ne, n_ep, cg, d = o_ref.shape
    in_refs, far_refs = rest[:IN_FRONT], rest[IN_FRONT:n_mb]
    near_ref, sent, pg, rows, sums, g_s, own_sem, row_send, row_recv, pg_sem, y_send, y_recv, out_sem = rest[n_mb:]
    t = g_s.shape[1] // 3
    e = lax.axis_index('ep')
    core = lax.rem(e, 2)
    chip = e // 2
    mate = e + 1 - 2 * core
    across = lax.rem(e + 2, n_ep)
    mate_across = lax.rem(mate + 2, n_ep)

    sent[:, :8] = place(ix_ref[...], sl_ref[...], 1 - chip, core, e, ne, cg)
    sent[:, 8:] = gt_ref[...]
    barrier = pltpu.get_barrier_semaphore()
    for dev in (mate, across):
        pl.semaphore_signal(barrier, inc=1, device_id={'ep': dev}, device_id_type=pl.DeviceIdType.MESH)
    pl.semaphore_wait(barrier, 2)

    gates = pltpu.make_async_remote_copy(sent, pg.at[pl.ds(0, n_mb)], pg_sem.at[0], pg_sem.at[1],
                                         device_id={'ep': across}, device_id_type=pl.DeviceIdType.MESH)
    gates.start()
    own, got = [], []
    for i in range(2 * n_mb):
        m = i % n_mb
        mine, theirs = (across, mate_across) if i < n_mb else (e, mate)
        got.append(pltpu.make_async_remote_copy(o_ref.at[m, :, theirs], rows.at[i, 1], row_send.at[i], row_recv.at[i],
                                                device_id={'ep': mate}, device_id_type=pl.DeviceIdType.MESH))
        own.append(pltpu.make_async_copy(o_ref.at[m, :, mine], rows.at[i, 0], own_sem.at[i]))
        got[i].start()
        own[i].start()
    pg[n_mb:, :8] = place(ix_ref[...], sl_ref[...], chip, core, e, ne, cg)
    pg[n_mb:, 8:] = gt_ref[...]
    gates.wait()

    def wait_rows(i):
        pltpu.make_async_copy(o_ref.at[0, :, 0], rows.at[i, 0], own_sem.at[i]).wait()
        pltpu.make_async_remote_copy(o_ref.at[0, :, 0], rows.at[i, 1], row_send.at[i], row_recv.at[i],
                                     device_id={'ep': mate}, device_id_type=pl.DeviceIdType.MESH).wait()

    def gates_of(i):
        gate_terms(pg[i, :8], pg[i, 8:], g_s, lax.rem(i, 2))

    def one(i, _):
        wait_rows(i)
        slot = lax.rem(i, 2)
        gates_of(lax.rem(i + 1, 2 * n_mb))
        for n in range(d // 256):
            c = slice(n * 256, (n + 1) * 256)
            r = jnp.dot(g_s[slot], rows[i, :, :, :, c].reshape(g_s.shape[2], 256), preferred_element_type=F32)
            sums[i, :, c] = (r[2 * t:] + r[t:2 * t]) + r[:t]
        return 0

    gates_of(0)
    first = []
    for i in range(IN_FRONT):
        one(i, 0)
        first.append(pltpu.make_async_remote_copy(sums.at[i], in_refs[i], y_send.at[i], y_recv.at[i],
                                                  device_id={'ep': across}, device_id_type=pl.DeviceIdType.MESH))
        first[i].start()
    lax.fori_loop(IN_FRONT, n_mb, one, 0)
    outs = [pltpu.make_async_copy(sums.at[m], far_refs[m - IN_FRONT], out_sem.at[m]) for m in range(IN_FRONT, n_mb)]
    for c in outs:
        c.start()
    lax.fori_loop(n_mb, 2 * n_mb, one, 0)
    near = pltpu.make_async_copy(sums.at[pl.ds(n_mb, n_mb)], near_ref, out_sem.at[0])
    near.start()
    for c in outs + [near] + first:
        c.wait()


def front(ix, sl, gt, o5):
    mb, ne, _, cg, d = o5.shape
    t = ix.shape[2]
    one = jax.ShapeDtypeStruct((t, d), F32)
    any_ = pl.BlockSpec(memory_space=pl.ANY)
    vm = pl.BlockSpec(memory_space=pltpu.VMEM)
    dma = pltpu.SemaphoreType.DMA
    return pl.pallas_call(
        front_kernel, name="front",
        in_specs=[vm, vm, vm, any_], out_specs=[any_] * (mb + 1),
        out_shape=[one] * mb + [jax.ShapeDtypeStruct((mb, t, d), F32)],
        scratch_shapes=[pltpu.VMEM((mb, 16, t), F32), pltpu.VMEM((2 * mb, 16, t), F32), pltpu.VMEM((2 * mb, 2, ne, cg, d), BF16),
                        pltpu.VMEM((2 * mb, t, d), F32), pltpu.VMEM((2, 3 * t, 2 * ne * cg), BF16),
                        dma((2 * mb,)), dma((2 * mb,)), dma((2 * mb,)), dma((2,)), dma((IN_FRONT,)), dma((IN_FRONT,)), dma((mb,))],
        cost_estimate=pl.CostEstimate(flops=2 * 3 * t * 2 * ne * cg * d * 2 * mb, bytes_accessed=0, transcendentals=0),
        compiler_params=pltpu.CompilerParams(vmem_limit_bytes=VMEM_LIMIT, collective_id=0, has_side_effects=True))(ix, sl, gt, o5)


def attn(q, k, v, nb, keep):
    hs = q.shape[1] // 128
    f = 128
    blk = [(h, b) for h in range(hs) for b in range(nb)]

    def cut(t, h, b):
        return t[b * 128:(b + 1) * 128, h * f:(h + 1) * f]

    s = [lax.dot_general(cut(q, h, b), cut(k, h, b), NT, preferred_element_type=F32) for h, b in blk]
    s = [jnp.where(keep, x * (f ** -0.5), -1e30) for x in s]
    m = [jnp.max(x, axis=-1, keepdims=True) for x in s]
    p = [jnp.exp(x - y) for x, y in zip(s, m)]
    d = [jnp.sum(x, axis=-1, keepdims=True) for x in p]
    p = [x * (1.0 / y) for x, y in zip(p, d)]
    o = [jnp.dot(x, cut(v, h, b).astype(F32), preferred_element_type=F32).astype(BF16) for x, (h, b) in zip(p, blk)]
    return jnp.concatenate([jnp.concatenate(o[h * nb:(h + 1) * nb], axis=0) for h in range(hs)], axis=1)


def turn_kernel(c_ref, q_ref, k_ref, v_ref, o_ref, qt_ref, kt_ref, vt_ref, ot_ref, sem):
    step = pl.program_id(0)
    hc = ot_ref.shape[0]
    kb = q_ref.shape[0]
    copy = pltpu.make_async_copy(o_ref.at[pl.ds(c_ref[0] * hc, hc)], ot_ref, sem)

    @pl.when(step == 0)
    def _():
        copy.start()

    rows = pl.ds(pl.multiple_of(step * kb, kb), kb)
    for i, o in ((q_ref, qt_ref), (k_ref, kt_ref), (v_ref, vt_ref)):
        o[:, rows, :] = jnp.swapaxes(i[...], 0, 1)

    @pl.when(step == pl.num_programs(0) - 1)
    def _():
        copy.wait()


def turn(core, wq, wk, wv, wo):
    d, nh, f = wq.shape
    hc, kb = nh // 2, 128
    vm = pl.BlockSpec(memory_space=pltpu.VMEM)
    return pl.pallas_call(
        turn_kernel, name="turn",
        grid_spec=pltpu.PrefetchScalarGridSpec(
            num_scalar_prefetch=1, grid=(d // kb,),
            in_specs=[pl.BlockSpec((kb, hc, f), lambda i, c: (i, c[0], 0))] * 3 + [pl.BlockSpec(memory_space=pl.ANY)],
            out_specs=[vm] * 4, scratch_shapes=[pltpu.SemaphoreType.DMA]),
        out_shape=[jax.ShapeDtypeStruct((hc, d, f), BF16)] * 3 + [jax.ShapeDtypeStruct((hc, f, d), BF16)],
        cost_estimate=pl.CostEstimate(flops=10**10, bytes_accessed=4 * d * hc * f * 2, transcendentals=0),
        compiler_params=pltpu.CompilerParams(vmem_limit_bytes=16 * 2**20))(core, wq, wk, wv, wo)


def layer_kernel(u_ref, v_ref, w_ref, q_ref, k_ref, vw_ref, o_ref, mine_ref, mate_ref, x_s):
    half, d = u_ref.shape
    hc = q_ref.shape[0]
    nb = 2 * half // 128
    for j, r_ref in enumerate((u_ref, v_ref)):
        for b in range(half // 128):
            uf = r_ref[b * 128:(b + 1) * 128].astype(F32)
            r = lax.rsqrt(jnp.mean(uf * uf, axis=-1, keepdims=True) + EPS)
            x_s[j * half + b * 128:j * half + (b + 1) * 128] = (uf * r * w_ref[...]).astype(BF16)
    keep = lax.broadcasted_iota(jnp.int32, (128, 128), 0) >= lax.broadcasted_iota(jnp.int32, (128, 128), 1)

    def heads(i):
        at = i * HS

        def proj(ref):
            wt = jnp.concatenate([ref[at + j] for j in range(HS)], axis=1)
            return jnp.dot(x_s[...], wt, preferred_element_type=F32).astype(BF16)

        q, k, v = proj(q_ref), proj(k_ref), proj(vw_ref)
        a = attn(q, k, v, nb, keep)
        return jnp.dot(a, o_ref[pl.ds(at, HS)].reshape(a.shape[1], d), preferred_element_type=F32)

    mine_ref[...] = jnp.zeros_like(mine_ref)
    mate_ref[...] = jnp.zeros_like(mate_ref)

    def more(i, _):
        t = heads(i)
        mine_ref[...] += t[:half]
        mate_ref[...] += t[half:]
        return 0

    lax.fori_loop(0, hc // HS, more, 0)


def layer(u, v, w, wq, wk, wv, wo):
    m, d = u.shape
    hc, _, f = wq.shape
    vm = pl.BlockSpec(memory_space=pltpu.VMEM)
    return pl.pallas_call(
        layer_kernel, name="layer", in_specs=[vm] * 7, out_specs=[vm] * 2,
        scratch_shapes=[pltpu.VMEM((2 * m, d), BF16)],
        out_shape=[jax.ShapeDtypeStruct((m, d), F32)] * 2,
        cost_estimate=pl.CostEstimate(flops=2 * 2 * m * d * hc * f * 4 * 2, bytes_accessed=4 * d * hc * f * 2, transcendentals=0),
        compiler_params=pltpu.CompilerParams(vmem_limit_bytes=12 * 2**20))(u, v, w, wq, wk, wv, wo)


def solution(mesh):
    npp = mesh.shape['pp']
    nep = mesh.shape['ep']
    perm = [(i, (i + 1) % npp) for i in range(npp)]
    mate = [(i, i ^ 1) for i in range(nep)]
    across = [(i, i ^ 2) for i in range(nep)]
    tok = P(('data', 'pp'), None, 'ep', None, None)
    wsp = P('pp', None, None, None)

    def step(O, idx, slot, g, H, w, Wq, Wk, Wv, Wo):
        o = O[0]
        mb, ne, cap, d = o.shape
        cg = cap // nep
        o5 = o.reshape(mb, ne, nep, cg, d)
        e = lax.axis_index('ep')
        core = e % 2
        ix, sl, gt = (jnp.swapaxes(a[0][:, 0], 1, 2) for a in (idx, slot, g))

        *part, near = front(ix, sl, gt, o5)
        for m in range(IN_FRONT, mb):
            part[m] = lax.ppermute(part[m], 'ep', across)
        cs = jnp.reshape(core, (1,)).astype(jnp.int32)
        h = H[0][:, 0]
        z = [None] * mb

        def finish(m, near):
            return (h[m].astype(F32) + near[m] + part[m]).astype(BF16)

        def start(u):
            v = lax.ppermute(u, 'ep', mate)
            mine, other = layer(u, v, w, *wt)
            return u, mine, lax.ppermute(other, 'ep', mate)

        def end(u, mine, other):
            return (u.astype(F32) + (mine + other).astype(BF16).astype(F32)).astype(BF16)

        y = [finish(m, near) for m in range(IN_FRONT)]
        ws, y, near = lax.optimization_barrier(((Wq[0], Wk[0], Wv[0], Wo[0]), y, near))


        def shift(x):
            return lax.ppermute(x, 'pp', perm)

        u = [shift(y[m]) for m in range(IN_FRONT)]
        wt = turn(cs, *ws)
        wt, near = lax.optimization_barrier((wt, near))
        y = None
        for what, m in zip("FLFLFLFLFLL", (1, 0, 2, 1, 3, 2, 4, 3, 5, 4, 5)):
            if what == "F":
                y = finish(m, near)
                u.append(shift(y))
                continue
            late, _ = lax.optimization_barrier((u[m], y))
            q = start(late)
            mine, near = lax.optimization_barrier((q[1], near))
            y = mine
            if m > 0:
                prev, mine = lax.optimization_barrier((z[m - 1], mine))
                z[m - 1] = end(*prev)
            z[m] = (q[0], mine, q[2])
        z[mb - 1] = end(*z[mb - 1])
        return jnp.stack(z).reshape(1, mb, 1, H.shape[3], d)

    return jax.shard_map(step, mesh=mesh,
                      in_specs=(tok, tok, tok, tok, tok, P('pp', None), wsp, wsp, wsp, wsp),
                      out_specs=tok, check_vma=False)
```
